16 devices in a mesh: data: 16 (over z, y, x, core).
Axes of the slice: x: 2, y: 2, z: 2, core: 2. Of those that a mesh axis runs over, the one named last changes fastest.
Arguments:
- tokens: bfloat16 [65536, 768], P('data')
- targets: bfloat16 [65536, 768], P('data')
- w_in: bfloat16 [4, 768, 3072], replicated
- w_out: bfloat16 [4, 3072, 768], replicated
Outputs:
- output 1: float32 [4, 768, 3072], replicated
- output 2: float32 [4, 3072, 768], replicated
All inputs are finite; a program needn't handle non-finite values.
Results may differ from the reference program's by a relative error of at most 0.0147433.
Values are sent between devices in bfloat16 or wider.
A program may use at most 1 GiB of HBM per device.

```python
import math
import jax
import jax.numpy as jnp
from jax import lax

TOKENS_DEV = 4096
D_MODEL = 768
D_HIDDEN = 3072
LAYERS = 4
GROUP_SIZE = 16

TOTAL_TOKENS = TOKENS_DEV * GROUP_SIZE
TARGET_SCALE = 1.0 + 16.0 * math.sqrt(TOTAL_TOKENS / D_MODEL)
LOSS_COEF = 1.0 / (TARGET_SCALE * math.sqrt(TOTAL_TOKENS))


def setup_inputs(seed: int = 0) -> dict:
    root_key = jax.random.key(seed)
    key_tok, key_tgt, key_in, key_out = jax.random.split(root_key, 4)
    tokens = jax.random.normal(key_tok, (TOTAL_TOKENS, D_MODEL), jnp.float32)
    targets = TARGET_SCALE * jax.random.normal(key_tgt, (TOTAL_TOKENS, D_MODEL), jnp.float32)
    w_in = jax.random.normal(key_in, (LAYERS, D_MODEL, D_HIDDEN), jnp.float32) * D_MODEL ** -0.5
    w_out = jax.random.normal(key_out, (LAYERS, D_HIDDEN, D_MODEL), jnp.float32) * D_HIDDEN ** -0.5
    return {'tokens': tokens.astype(jnp.bfloat16), 'targets': targets.astype(jnp.bfloat16), 'w_in': w_in.astype(jnp.bfloat16), 'w_out': w_out.astype(jnp.bfloat16)}


def layer_forward(hidden, w_first, w_second):
    pre_act = jnp.dot(hidden, w_first, preferred_element_type=jnp.float32).astype(jnp.bfloat16)
    activ = jax.nn.gelu(pre_act.astype(jnp.float32)).astype(jnp.bfloat16)
    branch = jnp.dot(activ, w_second, preferred_element_type=jnp.float32)
    return (hidden.astype(jnp.float32) + branch).astype(jnp.bfloat16)


def shard_loss(weights, tok_rows, tgt_rows):
    def layer_body(hidden, layer_w):
        return layer_forward(hidden, layer_w[0], layer_w[1]), None
    h_last, _ = lax.scan(layer_body, tok_rows, weights)
    error_rows = h_last.astype(jnp.float32) - tgt_rows.astype(jnp.float32)
    return 0.5 * LOSS_COEF * jnp.sum(error_rows * error_rows)


def reference(tokens, targets, w_in, w_out):
    tok_shards = tokens.reshape(GROUP_SIZE, TOKENS_DEV, D_MODEL)
    tgt_shards = targets.reshape(GROUP_SIZE, TOKENS_DEV, D_MODEL)
    grad_fn = jax.grad(shard_loss)

    def accumulate(running, shard_rows):
        local_grads = grad_fn((w_in, w_out), shard_rows[0], shard_rows[1])
        return (running[0] + local_grads[0].astype(jnp.float32), running[1] + local_grads[1].astype(jnp.float32)), None

    zero_init = (jnp.zeros((LAYERS, D_MODEL, D_HIDDEN), jnp.float32), jnp.zeros((LAYERS, D_HIDDEN, D_MODEL), jnp.float32))
    summed, _ = lax.scan(accumulate, zero_init, (tok_shards, tgt_shards))
    return (summed[0], summed[1])
```

```python
import functools
import math
import jax
import jax.numpy as jnp
from jax import lax
from jax.experimental import pallas as pl
from jax.experimental.pallas import tpu as pltpu
from jax.sharding import PartitionSpec as P

MESH = pl.DeviceIdType.MESH
ROWS_BOTH = (((0,), (0,)), ((), ()))
COLS_BOTH = (((1,), (1,)), ((), ()))
F32 = jnp.float32
BF16 = jnp.bfloat16

GELU_C = math.sqrt(2.0 / math.pi)
GELU_CK = GELU_C * 0.044715

HC = 512
BLK = 256
MT = 512
NS = 3
NF = 5
DELAY = 2


def backward_kernel(axis, layers, *refs):
    (gh_hbm, *rest) = refs
    h_hbm, rest = rest[:layers], rest[layers:]
    u_hbm, rest = rest[:layers], rest[layers:]
    (win_hbm, wout_hbm, gin_hbm, gout_hbm,
     gh, hb, back, ub, wi, wo, acc_out, acc_in, grads, pair, sums, full, recv0, recv1, recv2,
     gh_sem, h_sem, u_sem, wi_sem, wo_sem,
     pair_send, pair_recv, rs_send, rs_recv, ag_send, ag_recv, fin_local, fin_send, fin_recv) = rest
    recvs = (recv0, recv1, recv2)
    tokens, width = gh.shape
    per_layer = win_hbm.shape[2] // HC
    chunks = layers * per_layer
    pieces = 2 * chunks

    me = lax.axis_index(axis)
    core = lax.rem(me, 2)
    bit = [lax.rem(me // (2 << d), 2) for d in range(3)]
    peer = [me + (1 - 2 * bit[d]) * (2 << d) for d in range(3)]
    mate = me + 1 - 2 * core

    barrier = pltpu.get_barrier_semaphore()
    for other in (mate, *peer):
        pl.semaphore_signal(barrier, inc=1, device_id=(other,), device_id_type=MESH)
    pl.semaphore_wait(barrier, 4)

    def axis_of(p, k):
        return (p + k) % 3

    def kept(p, k):
        off = 0
        for j in range(k + 1):
            off = off + bit[axis_of(p, j)] * (BLK >> (j + 1))
        return off

    def given(p, k):
        off = kept(p, k - 1) if k else 0
        return off + (1 - bit[axis_of(p, k)]) * (BLK >> (k + 1))

    def rows_at(off, size):
        return pl.ds(pl.multiple_of(off, 32), size)

    def pair_copy(n):
        return pltpu.make_async_remote_copy(
            src_ref=grads.at[lax.rem(n, 4), 1 - core], dst_ref=pair.at[lax.rem(n, 2)],
            send_sem=pair_send.at[lax.rem(n, 2)], recv_sem=pair_recv.at[lax.rem(n, 2)],
            device_id=(mate,), device_id_type=MESH)

    def rs_copy(n, k, p):
        size = BLK >> (k + 1)
        return pltpu.make_async_remote_copy(
            src_ref=sums.at[lax.rem(n, NS), p, rows_at(given(p, k), size)],
            dst_ref=recvs[k].at[lax.rem(n, 2), p],
            send_sem=rs_send.at[k, lax.rem(n, 2), p], recv_sem=rs_recv.at[k, lax.rem(n, 2), p],
            device_id=(peer[axis_of(p, k)],), device_id_type=MESH)

    def ag_copy(n, k, p):
        part = full.at[lax.rem(n, NF), p, rows_at(kept(p, k), BLK >> (k + 1))]
        return pltpu.make_async_remote_copy(
            src_ref=part, dst_ref=part,
            send_sem=ag_send.at[k, lax.rem(n, 2), p], recv_sem=ag_recv.at[k, lax.rem(n, 2), p],
            device_id=(peer[axis_of(p, k)],), device_id_type=MESH)

    def ag_wait(n, k, p):
        ag_copy(n, k, p).wait_send()
        part = full.at[lax.rem(n, NF), p, rows_at(given(p, k), BLK >> (k + 1))]
        pltpu.make_async_remote_copy(
            src_ref=part, dst_ref=part,
            send_sem=ag_send.at[k, lax.rem(n, 2), p], recv_sem=ag_recv.at[k, lax.rem(n, 2), p],
            device_id=(peer[axis_of(p, k)],), device_id_type=MESH).wait_recv()

    def fin_copies(n, p, is_in, owner):
        chunk = n // 2
        layer = layers - 1 - chunk // per_layer
        first = pl.multiple_of(lax.rem(chunk, per_layer) * HC + owner * BLK, BLK)
        if is_in:
            dst = gin_hbm.at[layer, pl.ds(p * BLK, BLK), pl.ds(first, BLK)]
        else:
            dst = gout_hbm.at[layer, pl.ds(first, BLK), pl.ds(p * BLK, BLK)]
        src = full.at[lax.rem(n, NF), p]
        slot = lax.rem(n, 2)

        def local():
            return pltpu.make_async_copy(src, dst, fin_local.at[slot, p])

        def remote():
            return pltpu.make_async_remote_copy(
                src_ref=src, dst_ref=dst, send_sem=fin_send.at[slot, p], recv_sem=fin_recv.at[slot, p],
                device_id=(mate,), device_id_type=MESH)
        return local, remote

    def stage(n, body):
        pl.when(jnp.logical_and(n >= 0, n < pieces))(lambda: body(n))

    def both_kinds(n, body):
        pl.when(lax.rem(n, 2) == 0)(lambda: body(False))
        pl.when(lax.rem(n, 2) == 1)(lambda: body(True))

    def add_received(n, k):
        for p in range(3):
            rs_copy(n, k, p).wait()
        for p in range(3):
            rows = rows_at(kept(p, k), BLK >> (k + 1))
            total = sums[lax.rem(n, NS), p, rows] + recvs[k][lax.rem(n, 2), p]
            if k == 2:
                full[lax.rem(n, NF), p, rows] = total
            else:
                sums[lax.rem(n, NS), p, rows] = total

    def halve_last(n):
        add_received(n, 2)

    def halve(k, n):
        add_received(n, k)
        for p in range(3):
            rs_copy(n, k + 1, p).start()

    def add_pair(n):
        pair_copy(n).wait()
        for p in range(3):
            sums[lax.rem(n, NS), p] = (grads[lax.rem(n, 4), core, p].astype(F32)
                                       + pair[lax.rem(n, 2), p].astype(F32))
        for p in range(3):
            rs_copy(n, 0, p).start()

    def halving_side(t):
        stage(t - DELAY - 4, halve_last)
        stage(t - DELAY - 3, functools.partial(halve, 1))
        stage(t - DELAY - 2, functools.partial(halve, 0))
        stage(t - DELAY - 1, add_pair)
        stage(t - DELAY, lambda n: pair_copy(n).start())

    def finish_wait(n):
        def body(is_in):
            for p in range(3):
                local, remote = fin_copies(n, p, is_in, core)
                local().wait()
                remote().wait_send()
                fin_copies(n, p, is_in, 1 - core)[1]().wait_recv()
        both_kinds(n, body)

    def finish_start(n):
        for p in range(3):
            ag_wait(n, 0, p)

        def body(is_in):
            for p in range(3):
                local, remote = fin_copies(n, p, is_in, core)
                remote().start()
                local().start()
        both_kinds(n, body)

    def double(k, n):
        for p in range(3):
            ag_wait(n, k + 1, p)
        for p in range(3):
            ag_copy(n, k, p).start()

    def double_first(n):
        for p in range(3):
            ag_copy(n, 2, p).start()

    def doubling_side(t):
        stage(t - DELAY - 8, finish_wait)
        stage(t - DELAY - 7, finish_start)
        stage(t - DELAY - 6, functools.partial(double, 0))
        stage(t - DELAY - 5, functools.partial(double, 1))
        stage(t - DELAY - 4, double_first)

    def chunk_copies(i, layer_refs):
        layer = layers - 1 - i // per_layer
        cols = pl.ds(pl.multiple_of(lax.rem(i, per_layer) * HC, HC), HC)
        slot = lax.rem(i, 2)
        return (pltpu.make_async_copy(layer_refs.at[:, cols], ub.at[slot], u_sem.at[slot]),
                pltpu.make_async_copy(win_hbm.at[layer, :, cols], wi.at[slot], wi_sem.at[slot]),
                pltpu.make_async_copy(wout_hbm.at[layer, cols, :], wo.at[slot], wo_sem.at[slot]))

    def start_chunk(i):
        for k in range(layers):
            @pl.when(layers - 1 - i // per_layer == k)
            def _():
                for copy in chunk_copies(i, u_hbm[k]):
                    copy.start()

    def start_hidden(j):
        for k in range(layers):
            @pl.when(layers - 1 - j == k)
            def _():
                pltpu.make_async_copy(h_hbm[k], hb.at[lax.rem(j, 2)], h_sem.at[lax.rem(j, 2)]).start()

    def tile(m, slot, hslot):
        rows = pl.ds(pl.multiple_of(m * MT, MT), MT)
        u = ub[slot, rows, :].astype(F32)
        u2 = u * u
        t = jnp.tanh(u * (GELU_C + GELU_CK * u2))
        cdf = 0.5 + 0.5 * t
        act = (u * cdf).astype(BF16)
        slope = cdf + (u * (1.0 - t * t)) * (0.5 * GELU_C + 1.5 * GELU_CK * u2)
        g = gh[rows, :]
        g_act = lax.dot_general(g, wo[slot], COLS_BOTH, preferred_element_type=F32).astype(BF16)
        acc_out[...] += lax.dot_general(act, g, ROWS_BOTH, preferred_element_type=F32)
        g_pre = (g_act.astype(F32) * slope).astype(BF16)
        acc_in[...] += lax.dot_general(hb[hslot, rows, :], g_pre, ROWS_BOTH, preferred_element_type=F32)
        back[rows, :] += lax.dot_general(g_pre, wi[slot], COLS_BOTH, preferred_element_type=F32)

    first_gh = pltpu.make_async_copy(gh_hbm, gh, gh_sem.at[0])
    first_gh.start()
    start_chunk(0)
    start_hidden(0)
    first_gh.wait()

    def chunk_step(i, carry):
        slot = lax.rem(i, 2)
        j = i // per_layer
        hslot = lax.rem(j, 2)

        @pl.when(i + 1 < chunks)
        def _():
            start_chunk(i + 1)

        @pl.when(lax.rem(i, per_layer) == 0)
        def _():
            pltpu.make_async_copy(h_hbm[0], hb.at[hslot], h_sem.at[hslot]).wait()

            @pl.when(j + 1 < layers)
            def _():
                start_hidden(j + 1)

            @pl.loop(0, tokens // MT)
            def _(m):
                back[pl.ds(pl.multiple_of(m * MT, MT), MT), :] = jnp.zeros((MT, width), F32)

        acc_out[...] = jnp.zeros_like(acc_out)
        acc_in[...] = jnp.zeros_like(acc_in)
        for copy in chunk_copies(i, u_hbm[0]):
            copy.wait()

        @pl.loop(0, 4)
        def _(q):
            t = 2 * i + q // 2
            pl.when(lax.rem(q, 2) == 0)(lambda: halving_side(t))
            pl.when(lax.rem(q, 2) == 1)(lambda: doubling_side(t))
            per_quarter = tokens // MT // 4

            @pl.loop(0, per_quarter)
            def _(m):
                tile(q * per_quarter + m, slot, hslot)

        n_out = lax.rem(2 * i, 4)
        for half in range(2):
            for p in range(3):
                grads[n_out, half, p] = acc_out[half * BLK:(half + 1) * BLK, p * BLK:(p + 1) * BLK].astype(BF16)
                grads[n_out + 1, half, p] = acc_in[p * BLK:(p + 1) * BLK, half * BLK:(half + 1) * BLK].astype(BF16)

        @pl.when(jnp.logical_and(lax.rem(i, per_layer) == per_layer - 1, i + 1 < chunks))
        def _():
            @pl.loop(0, tokens // MT)
            def _(m):
                rows = pl.ds(pl.multiple_of(m * MT, MT), MT)
                gh[rows, :] = gh[rows, :] + back[rows, :].astype(BF16)
        return carry

    lax.fori_loop(0, chunks, chunk_step, 0)

    def drain(t, carry):
        halving_side(t)
        doubling_side(t)
        return carry

    lax.fori_loop(pieces, pieces + DELAY + 8, drain, 0)


def copy_kernel(a_ref, b_ref, c_ref, d_ref):
    c_ref[...] = a_ref[...]
    d_ref[...] = b_ref[...]


def solution(mesh):
    axis = mesh.axis_names[0]

    def grad_program(tokens, targets, w_in, w_out):
        total_tokens, width = tokens.shape
        target_scale = 1.0 + 16.0 * math.sqrt(total_tokens / width)
        loss_coef = 1.0 / (target_scale * math.sqrt(total_tokens))
        layers, _, hidden_width = w_in.shape

        def device_step(tok_rows, tgt_rows, w_first, w_second):
            rows = tok_rows.shape[0]
            hidden = tok_rows
            saved_h, saved_u = [], []
            for layer in range(layers):
                pre = jnp.dot(hidden, w_first[layer], preferred_element_type=F32).astype(BF16)
                act = jax.nn.gelu(pre.astype(F32)).astype(BF16)
                saved_h.append(hidden)
                saved_u.append(pre)
                branch = jnp.dot(act, w_second[layer], preferred_element_type=F32)
                hidden = (hidden.astype(F32) + branch).astype(BF16)
            error = hidden.astype(F32) - tgt_rows.astype(F32)
            grad_h = (error * loss_coef).astype(BF16)

            any_spec = pl.BlockSpec(memory_space=pl.ANY)
            dma = pltpu.SemaphoreType.DMA
            flops = 8 * rows * width * hidden_width * layers
            summed_in, summed_out = pl.pallas_call(
                functools.partial(backward_kernel, axis, layers),
                out_shape=(jax.ShapeDtypeStruct(w_first.shape, F32), jax.ShapeDtypeStruct(w_second.shape, F32)),
                in_specs=[any_spec] * (3 + 2 * layers),
                out_specs=(any_spec, any_spec),
                scratch_shapes=[
                    pltpu.VMEM((rows, width), BF16),
                    pltpu.VMEM((2, rows, width), BF16),
                    pltpu.VMEM((rows, width), F32),
                    pltpu.VMEM((2, rows, HC), BF16),
                    pltpu.VMEM((2, width, HC), BF16),
                    pltpu.VMEM((2, HC, width), BF16),
                    pltpu.VMEM((HC, width), F32),
                    pltpu.VMEM((width, HC), F32),
                    pltpu.VMEM((4, 2, 3, BLK, BLK), BF16),
                    pltpu.VMEM((2, 3, BLK, BLK), BF16),
                    pltpu.VMEM((NS, 3, BLK, BLK), F32),
                    pltpu.VMEM((NF, 3, BLK, BLK), F32),
                    pltpu.VMEM((2, 3, BLK // 2, BLK), F32),
                    pltpu.VMEM((2, 3, BLK // 4, BLK), F32),
                    pltpu.VMEM((2, 3, BLK // 8, BLK), F32),
                    dma((1,)), dma((2,)), dma((2,)), dma((2,)), dma((2,)),
                    dma((2,)), dma((2,)),
                    dma((3, 2, 3)), dma((3, 2, 3)), dma((3, 2, 3)), dma((3, 2, 3)),
                    dma((2, 3)), dma((2, 3)), dma((2, 3)),
                ],
                compiler_params=pltpu.CompilerParams(
                    collective_id=0, has_side_effects=True, vmem_limit_bytes=67043328),
                cost_estimate=pl.CostEstimate(flops=flops, bytes_accessed=300 * 2**20, transcendentals=0),
                name="backward_allreduce",
            )(grad_h, *saved_h, *saved_u, w_first, w_second)

            steps = 3 * layers
            in_block = pl.BlockSpec((1, width // 3, hidden_width), lambda s: (s // 3, s % 3, 0))
            out_block = pl.BlockSpec((1, hidden_width // 3, width), lambda s: (s // 3, s % 3, 0))
            return pl.pallas_call(
                copy_kernel,
                grid=(steps,),
                out_shape=(jax.ShapeDtypeStruct(w_first.shape, F32), jax.ShapeDtypeStruct(w_second.shape, F32)),
                in_specs=[in_block, out_block],
                out_specs=(in_block, out_block),
                compiler_params=pltpu.CompilerParams(vmem_limit_bytes=60 * 2**20),
                name="copy_out",
            )(summed_in, summed_out)

        return jax.shard_map(device_step, mesh=mesh, in_specs=(P(axis), P(axis), P(), P()), out_specs=(P(), P()), check_vma=False)(tokens, targets, w_in, w_out)

    return grad_program
```

```python
import functools
import math
import jax
import jax.numpy as jnp
from jax import lax
from jax.experimental import pallas as pl
from jax.experimental.pallas import tpu as pltpu
from jax.sharding import PartitionSpec as P

MESH = pl.DeviceIdType.MESH
ROWS_BOTH = (((0,), (0,)), ((), ()))
COLS_BOTH = (((1,), (1,)), ((), ()))
F32 = jnp.float32
BF16 = jnp.bfloat16

GELU_C = math.sqrt(2.0 / math.pi)
GELU_CK = GELU_C * 0.044715

HC = 512
BLK = 256
MT = 512
NS = 3
NF = 5
FC = 3072
FT = 512
DELAY = 2


def backward_kernel(axis, layers, *refs):
    (gh_hbm, *rest) = refs
    h_hbm, rest = rest[:layers], rest[layers:]
    u_hbm, rest = rest[:layers], rest[layers:]
    (win_hbm, wout_hbm, gin_hbm, gout_hbm,
     gh, hb, back, ub, wi, wo, acc_out, acc_in, grads, pair, sums, full, recv0, recv1, recv2,
     gh_sem, h_sem, u_sem, wi_sem, wo_sem,
     pair_send, pair_recv, rs_send, rs_recv, ag_send, ag_recv, fin_local, fin_send, fin_recv) = rest
    recvs = (recv0, recv1, recv2)
    tokens, width = gh.shape
    per_layer = win_hbm.shape[2] // HC
    chunks = layers * per_layer
    pieces = 2 * chunks

    me = lax.axis_index(axis)
    core = lax.rem(me, 2)
    bit = [lax.rem(me // (2 << d), 2) for d in range(3)]
    peer = [me + (1 - 2 * bit[d]) * (2 << d) for d in range(3)]
    mate = me + 1 - 2 * core

    barrier = pltpu.get_barrier_semaphore()
    for other in (mate, *peer):
        pl.semaphore_signal(barrier, inc=1, device_id=(other,), device_id_type=MESH)
    pl.semaphore_wait(barrier, 4)

    def axis_of(p, k):
        return (p + k) % 3

    def kept(p, k):
        off = 0
        for j in range(k + 1):
            off = off + bit[axis_of(p, j)] * (BLK >> (j + 1))
        return off

    def given(p, k):
        off = kept(p, k - 1) if k else 0
        return off + (1 - bit[axis_of(p, k)]) * (BLK >> (k + 1))

    def rows_at(off, size):
        return pl.ds(pl.multiple_of(off, 32), size)

    def pair_copy(n):
        return pltpu.make_async_remote_copy(
            src_ref=grads.at[lax.rem(n, 4), 1 - core], dst_ref=pair.at[lax.rem(n, 2)],
            send_sem=pair_send.at[lax.rem(n, 2)], recv_sem=pair_recv.at[lax.rem(n, 2)],
            device_id=(mate,), device_id_type=MESH)

    def rs_copy(n, k, p):
        size = BLK >> (k + 1)
        return pltpu.make_async_remote_copy(
            src_ref=sums.at[lax.rem(n, NS), p, rows_at(given(p, k), size)],
            dst_ref=recvs[k].at[lax.rem(n, 2), p],
            send_sem=rs_send.at[k, lax.rem(n, 2), p], recv_sem=rs_recv.at[k, lax.rem(n, 2), p],
            device_id=(peer[axis_of(p, k)],), device_id_type=MESH)

    def ag_copy(n, k, p):
        part = full.at[lax.rem(n, NF), p, rows_at(kept(p, k), BLK >> (k + 1))]
        return pltpu.make_async_remote_copy(
            src_ref=part, dst_ref=part,
            send_sem=ag_send.at[k, lax.rem(n, 2), p], recv_sem=ag_recv.at[k, lax.rem(n, 2), p],
            device_id=(peer[axis_of(p, k)],), device_id_type=MESH)

    def ag_wait(n, k, p):
        ag_copy(n, k, p).wait_send()
        part = full.at[lax.rem(n, NF), p, rows_at(given(p, k), BLK >> (k + 1))]
        pltpu.make_async_remote_copy(
            src_ref=part, dst_ref=part,
            send_sem=ag_send.at[k, lax.rem(n, 2), p], recv_sem=ag_recv.at[k, lax.rem(n, 2), p],
            device_id=(peer[axis_of(p, k)],), device_id_type=MESH).wait_recv()

    def fin_copies(n, p, is_in, owner):
        chunk = n // 2
        layer = layers - 1 - chunk // per_layer
        first = pl.multiple_of(lax.rem(chunk, per_layer) * HC + owner * BLK, BLK)
        if is_in:
            dst = gin_hbm.at[layer, pl.ds(p * BLK, BLK), pl.ds(first, BLK)]
        else:
            dst = gout_hbm.at[layer, pl.ds(first, BLK), pl.ds(p * BLK, BLK)]
        src = full.at[lax.rem(n, NF), p]
        slot = lax.rem(n, 2)

        def local():
            return pltpu.make_async_copy(src, dst, fin_local.at[slot, p])

        def remote():
            return pltpu.make_async_remote_copy(
                src_ref=src, dst_ref=dst, send_sem=fin_send.at[slot, p], recv_sem=fin_recv.at[slot, p],
                device_id=(mate,), device_id_type=MESH)
        return local, remote

    def stage(n, body):
        pl.when(jnp.logical_and(n >= 0, n < pieces))(lambda: body(n))

    def both_kinds(n, body):
        pl.when(lax.rem(n, 2) == 0)(lambda: body(False))
        pl.when(lax.rem(n, 2) == 1)(lambda: body(True))

    def add_received(n, k):
        for p in range(3):
            rs_copy(n, k, p).wait()
        for p in range(3):
            rows = rows_at(kept(p, k), BLK >> (k + 1))
            total = sums[lax.rem(n, NS), p, rows] + recvs[k][lax.rem(n, 2), p]
            if k == 2:
                full[lax.rem(n, NF), p, rows] = total
            else:
                sums[lax.rem(n, NS), p, rows] = total

    def halve_last(n):
        add_received(n, 2)

    def halve(k, n):
        add_received(n, k)
        for p in range(3):
            rs_copy(n, k + 1, p).start()

    def add_pair(n):
        pair_copy(n).wait()
        for p in range(3):
            sums[lax.rem(n, NS), p] = (grads[lax.rem(n, 4), core, p].astype(F32)
                                       + pair[lax.rem(n, 2), p].astype(F32))
        for p in range(3):
            rs_copy(n, 0, p).start()

    def halving_side(t):
        stage(t - DELAY - 4, halve_last)
        stage(t - DELAY - 3, functools.partial(halve, 1))
        stage(t - DELAY - 2, functools.partial(halve, 0))
        stage(t - DELAY - 1, add_pair)
        stage(t - DELAY, lambda n: pair_copy(n).start())

    def finish_wait(n):
        def body(is_in):
            for p in range(3):
                local, remote = fin_copies(n, p, is_in, core)
                local().wait()
                remote().wait_send()
                fin_copies(n, p, is_in, 1 - core)[1]().wait_recv()
        both_kinds(n, body)

    def finish_start(n):
        for p in range(3):
            ag_wait(n, 0, p)

        def body(is_in):
            for p in range(3):
                local, remote = fin_copies(n, p, is_in, core)
                remote().start()
                local().start()
        both_kinds(n, body)

    def double(k, n):
        for p in range(3):
            ag_wait(n, k + 1, p)
        for p in range(3):
            ag_copy(n, k, p).start()

    def double_first(n):
        for p in range(3):
            ag_copy(n, 2, p).start()

    def doubling_side(t):
        stage(t - DELAY - 8, finish_wait)
        stage(t - DELAY - 7, finish_start)
        stage(t - DELAY - 6, functools.partial(double, 0))
        stage(t - DELAY - 5, functools.partial(double, 1))
        stage(t - DELAY - 4, double_first)

    def chunk_copies(i, layer_refs):
        layer = layers - 1 - i // per_layer
        cols = pl.ds(pl.multiple_of(lax.rem(i, per_layer) * HC, HC), HC)
        slot = lax.rem(i, 2)
        return (pltpu.make_async_copy(layer_refs.at[:, cols], ub.at[slot], u_sem.at[slot]),
                pltpu.make_async_copy(win_hbm.at[layer, :, cols], wi.at[slot], wi_sem.at[slot]),
                pltpu.make_async_copy(wout_hbm.at[layer, cols, :], wo.at[slot], wo_sem.at[slot]))

    def start_chunk(i):
        for k in range(layers):
            @pl.when(layers - 1 - i // per_layer == k)
            def _():
                for copy in chunk_copies(i, u_hbm[k]):
                    copy.start()

    def start_hidden(j):
        for k in range(layers):
            @pl.when(layers - 1 - j == k)
            def _():
                pltpu.make_async_copy(h_hbm[k], hb.at[lax.rem(j, 2)], h_sem.at[lax.rem(j, 2)]).start()

    def tile(m, slot, hslot):
        rows = pl.ds(pl.multiple_of(m * MT, MT), MT)
        u = ub[slot, rows, :].astype(F32)
        u2 = u * u
        t = jnp.tanh(u * (GELU_C + GELU_CK * u2))
        cdf = 0.5 + 0.5 * t
        act = (u * cdf).astype(BF16)
        slope = cdf + (u * (1.0 - t * t)) * (0.5 * GELU_C + 1.5 * GELU_CK * u2)
        g = gh[rows, :]
        g_act = lax.dot_general(g, wo[slot], COLS_BOTH, preferred_element_type=F32).astype(BF16)
        acc_out[...] += lax.dot_general(act, g, ROWS_BOTH, preferred_element_type=F32)
        g_pre = (g_act.astype(F32) * slope).astype(BF16)
        acc_in[...] += lax.dot_general(hb[hslot, rows, :], g_pre, ROWS_BOTH, preferred_element_type=F32)
        back[rows, :] += lax.dot_general(g_pre, wi[slot], COLS_BOTH, preferred_element_type=F32)

    first_gh = pltpu.make_async_copy(gh_hbm, gh, gh_sem.at[0])
    first_gh.start()
    start_chunk(0)
    start_hidden(0)
    first_gh.wait()

    def chunk_step(i, carry):
        slot = lax.rem(i, 2)
        j = i // per_layer
        hslot = lax.rem(j, 2)

        @pl.when(i + 1 < chunks)
        def _():
            start_chunk(i + 1)

        @pl.when(lax.rem(i, per_layer) == 0)
        def _():
            pltpu.make_async_copy(h_hbm[0], hb.at[hslot], h_sem.at[hslot]).wait()

            @pl.when(j + 1 < layers)
            def _():
                start_hidden(j + 1)

            @pl.loop(0, tokens // MT)
            def _(m):
                back[pl.ds(pl.multiple_of(m * MT, MT), MT), :] = jnp.zeros((MT, width), F32)

        acc_out[...] = jnp.zeros_like(acc_out)
        acc_in[...] = jnp.zeros_like(acc_in)
        for copy in chunk_copies(i, u_hbm[0]):
            copy.wait()

        @pl.loop(0, 4)
        def _(q):
            t = 2 * i + q // 2
            pl.when(lax.rem(q, 2) == 0)(lambda: halving_side(t))
            pl.when(lax.rem(q, 2) == 1)(lambda: doubling_side(t))
            per_quarter = tokens // MT // 4

            @pl.loop(0, per_quarter)
            def _(m):
                tile(q * per_quarter + m, slot, hslot)

        n_out = lax.rem(2 * i, 4)
        for half in range(2):
            for p in range(3):
                grads[n_out, half, p] = acc_out[half * BLK:(half + 1) * BLK, p * BLK:(p + 1) * BLK].astype(BF16)
                grads[n_out + 1, half, p] = acc_in[p * BLK:(p + 1) * BLK, half * BLK:(half + 1) * BLK].astype(BF16)

        @pl.when(jnp.logical_and(lax.rem(i, per_layer) == per_layer - 1, i + 1 < chunks))
        def _():
            @pl.loop(0, tokens // MT)
            def _(m):
                rows = pl.ds(pl.multiple_of(m * MT, MT), MT)
                gh[rows, :] = gh[rows, :] + back[rows, :].astype(BF16)
        return carry

    lax.fori_loop(0, chunks, chunk_step, 0)

    def drain(t, carry):
        halving_side(t)
        doubling_side(t)
        return carry

    lax.fori_loop(pieces, pieces + DELAY + 8, drain, 0)


def forward_kernel(layers, coef, *refs):
    (x_hbm, t_hbm, win_hbm, wout_hbm), rest = refs[:4], refs[4:]
    gh_hbm, rest = rest[0], rest[1:]
    h_hbm, rest = rest[:layers - 1], rest[layers - 1:]
    u_hbm, rest = rest[:layers], rest[layers:]
    win, wout, hid, branch, ubuf, hbuf, tbuf, gbuf, w_sem, x_sem, t_sem, u_sem, h_sem, g_sem = rest
    tokens = x_hbm.shape[0]
    chunks = win.shape[2] // FC
    tiles = tokens // FT

    def weight_copies(k):
        return (pltpu.make_async_copy(win_hbm.at[k], win.at[k], w_sem.at[k, 0]),
                pltpu.make_async_copy(wout_hbm.at[k], wout.at[k], w_sem.at[k, 1]))

    def tile_rows(r):
        return pl.ds(pl.multiple_of(r * FT, FT), FT)

    def load_x(r):
        return pltpu.make_async_copy(x_hbm.at[tile_rows(r)], hid.at[lax.rem(r, 2)], x_sem.at[lax.rem(r, 2)])

    def load_t(r):
        return pltpu.make_async_copy(t_hbm.at[tile_rows(r)], tbuf, t_sem.at[0])

    def step_of(r, k, c):
        return (r * layers + k) * chunks + c

    def store_u(r, k, c):
        cols = pl.ds(pl.multiple_of(c * FC, FC), FC)
        slot = lax.rem(step_of(r, k, c), 2)
        return pltpu.make_async_copy(ubuf.at[slot], u_hbm[k].at[tile_rows(r), cols], u_sem.at[slot])

    def store_h(r, k):
        return pltpu.make_async_copy(hbuf.at[k % 2], h_hbm[k].at[tile_rows(r)], h_sem.at[k % 2])

    def store_g(r):
        return pltpu.make_async_copy(gbuf, gh_hbm.at[tile_rows(r)], g_sem.at[0])

    load_x(0).start()
    for k in range(layers):
        for copy in weight_copies(k):
            copy.start()

    @pl.loop(0, tiles)
    def _(r):
        cur = lax.rem(r, 2)
        load_x(r).wait()
        load_t(r).start()

        @pl.when(r + 1 < tiles)
        def _():
            load_x(r + 1).start()

        for k in range(layers):
            @pl.when(r == 0)
            def _():
                for copy in weight_copies(k):
                    copy.wait()

            branch[...] = hid[cur].astype(F32)

            @pl.loop(0, chunks)
            def _(c):
                @pl.when(step_of(r, k, c) >= 2)
                def _():
                    store_u(r, k, c).wait()
                cols = pl.ds(pl.multiple_of(c * FC, FC), FC)
                pre = jnp.dot(hid[cur], win[k, :, cols], preferred_element_type=F32).astype(BF16)
                ubuf[lax.rem(step_of(r, k, c), 2)] = pre
                u = pre.astype(F32)
                t = jnp.tanh(u * (GELU_C + GELU_CK * (u * u)))
                act = (u * (0.5 + 0.5 * t)).astype(BF16)
                branch[...] += jnp.dot(act, wout[k, cols, :], preferred_element_type=F32)
                store_u(r, k, c).start()

            new = branch[...].astype(BF16)
            if k < layers - 1:
                @pl.when(r * layers + k >= 2)
                def _():
                    store_h(r, k).wait()
                hid[cur] = new
                hbuf[k % 2] = new
                store_h(r, k).start()
            else:
                load_t(r).wait()

                @pl.when(r > 0)
                def _():
                    store_g(r).wait()
                gbuf[...] = ((new.astype(F32) - tbuf[...].astype(F32)) * coef).astype(BF16)
                store_g(r).start()

    for slot in range(2):
        cols = pl.ds(0, FC)
        pltpu.make_async_copy(ubuf.at[slot], u_hbm[0].at[pl.ds(0, FT), cols], u_sem.at[slot]).wait()
    for k in range(min(2, layers - 1)):
        store_h(tiles - 1, k).wait()
    store_g(tiles - 1).wait()


def copy_kernel(a_ref, b_ref, c_ref, d_ref):
    c_ref[...] = a_ref[...]
    d_ref[...] = b_ref[...]


def solution(mesh):
    axis = mesh.axis_names[0]

    def grad_program(tokens, targets, w_in, w_out):
        total_tokens, width = tokens.shape
        target_scale = 1.0 + 16.0 * math.sqrt(total_tokens / width)
        loss_coef = 1.0 / (target_scale * math.sqrt(total_tokens))
        layers, _, hidden_width = w_in.shape

        def device_step(tok_rows, tgt_rows, w_first, w_second):
            rows = tok_rows.shape[0]
            any_spec = pl.BlockSpec(memory_space=pl.ANY)
            dma = pltpu.SemaphoreType.DMA
            row_shape = jax.ShapeDtypeStruct((rows, width), BF16)
            pre_shape = jax.ShapeDtypeStruct((rows, hidden_width), BF16)
            forward = pl.pallas_call(
                functools.partial(forward_kernel, layers, loss_coef),
                out_shape=[row_shape] * layers + [pre_shape] * layers,
                in_specs=[any_spec] * 4,
                out_specs=[any_spec] * (2 * layers),
                scratch_shapes=[
                    pltpu.VMEM(w_first.shape, BF16), pltpu.VMEM(w_second.shape, BF16),
                    pltpu.VMEM((2, FT, width), BF16), pltpu.VMEM((FT, width), F32),
                    pltpu.VMEM((2, FT, FC), BF16), pltpu.VMEM((2, FT, width), BF16),
                    pltpu.VMEM((FT, width), BF16), pltpu.VMEM((FT, width), BF16),
                    dma((layers, 2)), dma((2,)), dma((1,)), dma((2,)), dma((2,)), dma((1,)),
                ],
                compiler_params=pltpu.CompilerParams(vmem_limit_bytes=67043328),
                cost_estimate=pl.CostEstimate(flops=4 * rows * width * hidden_width * layers,
                                              bytes_accessed=200 * 2**20, transcendentals=0),
                name="forward",
            )(tok_rows, tgt_rows, w_first, w_second)
            grad_h, saved_h, saved_u = forward[0], [tok_rows, *forward[1:layers]], forward[layers:]

            flops = 8 * rows * width * hidden_width * layers
            summed_in, summed_out = pl.pallas_call(
                functools.partial(backward_kernel, axis, layers),
                out_shape=(jax.ShapeDtypeStruct(w_first.shape, F32), jax.ShapeDtypeStruct(w_second.shape, F32)),
                in_specs=[any_spec] * (3 + 2 * layers),
                out_specs=(any_spec, any_spec),
                scratch_shapes=[
                    pltpu.VMEM((rows, width), BF16),
                    pltpu.VMEM((2, rows, width), BF16),
                    pltpu.VMEM((rows, width), F32),
                    pltpu.VMEM((2, rows, HC), BF16),
                    pltpu.VMEM((2, width, HC), BF16),
                    pltpu.VMEM((2, HC, width), BF16),
                    pltpu.VMEM((HC, width), F32),
                    pltpu.VMEM((width, HC), F32),
                    pltpu.VMEM((4, 2, 3, BLK, BLK), BF16),
                    pltpu.VMEM((2, 3, BLK, BLK), BF16),
                    pltpu.VMEM((NS, 3, BLK, BLK), F32),
                    pltpu.VMEM((NF, 3, BLK, BLK), F32),
                    pltpu.VMEM((2, 3, BLK // 2, BLK), F32),
                    pltpu.VMEM((2, 3, BLK // 4, BLK), F32),
                    pltpu.VMEM((2, 3, BLK // 8, BLK), F32),
                    dma((1,)), dma((2,)), dma((2,)), dma((2,)), dma((2,)),
                    dma((2,)), dma((2,)),
                    dma((3, 2, 3)), dma((3, 2, 3)), dma((3, 2, 3)), dma((3, 2, 3)),
                    dma((2, 3)), dma((2, 3)), dma((2, 3)),
                ],
                compiler_params=pltpu.CompilerParams(
                    collective_id=0, has_side_effects=True, vmem_limit_bytes=67043328),
                cost_estimate=pl.CostEstimate(flops=flops, bytes_accessed=300 * 2**20, transcendentals=0),
                name="backward_allreduce",
            )(grad_h, *saved_h, *saved_u, w_first, w_second)

            steps = 3 * layers
            in_block = pl.BlockSpec((1, width // 3, hidden_width), lambda s: (s // 3, s % 3, 0))
            out_block = pl.BlockSpec((1, hidden_width // 3, width), lambda s: (s // 3, s % 3, 0))
            return pl.pallas_call(
                copy_kernel,
                grid=(steps,),
                out_shape=(jax.ShapeDtypeStruct(w_first.shape, F32), jax.ShapeDtypeStruct(w_second.shape, F32)),
                in_specs=[in_block, out_block],
                out_specs=(in_block, out_block),
                compiler_params=pltpu.CompilerParams(vmem_limit_bytes=60 * 2**20),
                name="copy_out",
            )(summed_in, summed_out)

        return jax.shard_map(device_step, mesh=mesh, in_specs=(P(axis), P(axis), P(), P()), out_specs=(P(), P()), check_vma=False)(tokens, targets, w_in, w_out)

    return grad_program
```

```python
import functools
import math
import jax
import jax.numpy as jnp
from jax import lax
from jax.experimental import pallas as pl
from jax.experimental.pallas import tpu as pltpu
from jax.sharding import PartitionSpec as P

MESH = pl.DeviceIdType.MESH
ROWS_BOTH = (((0,), (0,)), ((), ()))
COLS_BOTH = (((1,), (1,)), ((), ()))
F32 = jnp.float32
BF16 = jnp.bfloat16

GELU_C = math.sqrt(2.0 / math.pi)
GELU_CK = GELU_C * 0.044715

HC = 512
BLK = 256
MT = 1024
NS = 3
NF = 5
FC = 3072
FT = 512
DELAY = 2


def backward_kernel(axis, layers, *refs):
    (gh_hbm, *rest) = refs
    h_hbm, rest = rest[:layers], rest[layers:]
    u_hbm, rest = rest[:layers], rest[layers:]
    (win_hbm, wout_hbm, gin_hbm, gout_hbm,
     gh, hb, back, ub, wi, wo, acc_out, acc_in, grads, pair, sums, away, full, recv0, recv1, recv2,
     first_sem, h_sem, u_sem, wi_sem, wo_sem,
     pair_send, pair_recv, rs_send, rs_recv, ag_send, ag_recv, fin_local, fin_send, fin_recv) = rest
    recvs = (recv0, recv1, recv2)
    tokens, width = gh.shape
    per_layer = win_hbm.shape[2] // HC
    chunks = layers * per_layer
    pieces = 2 * chunks

    me = lax.axis_index(axis)
    core = lax.rem(me, 2)
    bit = [lax.rem(me // (2 << d), 2) for d in range(3)]
    peer = [me + (1 - 2 * bit[d]) * (2 << d) for d in range(3)]
    mate = me + 1 - 2 * core

    barrier = pltpu.get_barrier_semaphore()
    for other in (mate, *peer):
        pl.semaphore_signal(barrier, inc=1, device_id=(other,), device_id_type=MESH)
    pl.semaphore_wait(barrier, 4)

    def axis_of(p, k):
        return (p + k) % 3

    def kept(p, k):
        off = 0
        for j in range(k + 1):
            off = off + bit[axis_of(p, j)] * (BLK >> (j + 1))
        return off

    def given(p, k):
        off = kept(p, k - 1) if k else 0
        return off + (1 - bit[axis_of(p, k)]) * (BLK >> (k + 1))

    def rows_at(off, size):
        return pl.ds(pl.multiple_of(off, 32), size)

    def pair_copy(n):
        return pltpu.make_async_remote_copy(
            src_ref=grads.at[lax.rem(n, 3), 1 - core], dst_ref=pair.at[lax.rem(n, 2)],
            send_sem=pair_send.at[lax.rem(n, 2)], recv_sem=pair_recv.at[lax.rem(n, 2)],
            device_id=(mate,), device_id_type=MESH)

    def rs_copy(n, k, p):
        size = BLK >> (k + 1)
        src = sums.at[lax.rem(n, NS), p, rows_at(given(p, k) - kept(p, 0), size)] if k else away.at[p]
        return pltpu.make_async_remote_copy(
            src_ref=src,
            dst_ref=recvs[k].at[lax.rem(n, 2), p],
            send_sem=rs_send.at[k, lax.rem(n, 2), p], recv_sem=rs_recv.at[k, lax.rem(n, 2), p],
            device_id=(peer[axis_of(p, k)],), device_id_type=MESH)

    def ag_copy(n, k, p):
        part = full.at[lax.rem(n, NF), p, rows_at(kept(p, k), BLK >> (k + 1))]
        return pltpu.make_async_remote_copy(
            src_ref=part, dst_ref=part,
            send_sem=ag_send.at[k, lax.rem(n, 2), p], recv_sem=ag_recv.at[k, lax.rem(n, 2), p],
            device_id=(peer[axis_of(p, k)],), device_id_type=MESH)

    def ag_wait(n, k, p):
        ag_copy(n, k, p).wait_send()
        part = full.at[lax.rem(n, NF), p, rows_at(given(p, k), BLK >> (k + 1))]
        pltpu.make_async_remote_copy(
            src_ref=part, dst_ref=part,
            send_sem=ag_send.at[k, lax.rem(n, 2), p], recv_sem=ag_recv.at[k, lax.rem(n, 2), p],
            device_id=(peer[axis_of(p, k)],), device_id_type=MESH).wait_recv()

    def fin_copies(n, p, is_in, owner):
        chunk = n // 2
        layer = layers - 1 - chunk // per_layer
        first = pl.multiple_of(lax.rem(chunk, per_layer) * HC + owner * BLK, BLK)
        if is_in:
            dst = gin_hbm.at[layer, pl.ds(p * BLK, BLK), pl.ds(first, BLK)]
        else:
            dst = gout_hbm.at[layer, pl.ds(first, BLK), pl.ds(p * BLK, BLK)]
        src = full.at[lax.rem(n, NF), p]
        slot = lax.rem(n, 2)

        def local():
            return pltpu.make_async_copy(src, dst, fin_local.at[slot, p])

        def remote():
            return pltpu.make_async_remote_copy(
                src_ref=src, dst_ref=dst, send_sem=fin_send.at[slot, p], recv_sem=fin_recv.at[slot, p],
                device_id=(mate,), device_id_type=MESH)
        return local, remote

    def stage(n, body):
        pl.when(jnp.logical_and(n >= 0, n < pieces))(lambda: body(n))

    def both_kinds(n, body):
        pl.when(lax.rem(n, 2) == 0)(lambda: body(False))
        pl.when(lax.rem(n, 2) == 1)(lambda: body(True))

    def add_received(n, k):
        for p in range(3):
            rs_copy(n, k, p).wait()
        for p in range(3):
            size = BLK >> (k + 1)
            rows = rows_at(kept(p, k) - kept(p, 0), size)
            total = sums[lax.rem(n, NS), p, rows] + recvs[k][lax.rem(n, 2), p]
            if k == 2:
                full[lax.rem(n, NF), p, rows_at(kept(p, k), size)] = total
            else:
                sums[lax.rem(n, NS), p, rows] = total

    def halve_last(n):
        add_received(n, 2)

    def halve(k, n):
        add_received(n, k)
        for p in range(3):
            rs_copy(n, k + 1, p).start()

    def add_pair(n):
        pair_copy(n).wait()
        for p in range(3):
            for rows, dst in ((kept(p, 0), sums.at[lax.rem(n, NS), p]), (given(p, 0), away.at[p])):
                rows = pl.ds(pl.multiple_of(rows, BLK // 2), BLK // 2)
                dst[...] = (grads[lax.rem(n, 3), core, p, rows].astype(F32)
                            + pair[lax.rem(n, 2), p, rows].astype(F32))
        for p in range(3):
            rs_copy(n, 0, p).start()

    def halving_side(t):
        stage(t - DELAY - 4, halve_last)
        stage(t - DELAY - 3, functools.partial(halve, 1))
        stage(t - DELAY - 2, functools.partial(halve, 0))
        stage(t - DELAY - 1, add_pair)
        stage(t - DELAY, lambda n: pair_copy(n).start())

    def finish_wait(n):
        def body(is_in):
            for p in range(3):
                local, remote = fin_copies(n, p, is_in, core)
                local().wait()
                remote().wait_send()
                fin_copies(n, p, is_in, 1 - core)[1]().wait_recv()
        both_kinds(n, body)

    def finish_start(n):
        for p in range(3):
            ag_wait(n, 0, p)

        def body(is_in):
            for p in range(3):
                local, remote = fin_copies(n, p, is_in, core)
                remote().start()
                local().start()
        both_kinds(n, body)

    def double(k, n):
        for p in range(3):
            ag_wait(n, k + 1, p)
        for p in range(3):
            ag_copy(n, k, p).start()

    def double_first(n):
        for p in range(3):
            ag_copy(n, 2, p).start()

    def doubling_side(t):
        stage(t - DELAY - 8, finish_wait)
        stage(t - DELAY - 7, finish_start)
        stage(t - DELAY - 6, functools.partial(double, 0))
        stage(t - DELAY - 5, functools.partial(double, 1))
        stage(t - DELAY - 4, double_first)

    def pre_of(i, layer_refs):
        cols = pl.ds(pl.multiple_of(lax.rem(i, per_layer) * HC, HC), HC)
        return pltpu.make_async_copy(layer_refs.at[:, cols], ub.at[lax.rem(i, 2)], u_sem.at[lax.rem(i, 2)])

    def weights_of(i):
        layer = layers - 1 - i // per_layer
        cols = pl.ds(pl.multiple_of(lax.rem(i, per_layer) * HC, HC), HC)
        slot = lax.rem(i, 2)
        return (pltpu.make_async_copy(win_hbm.at[layer, :, cols], wi.at[slot], wi_sem.at[slot]),
                pltpu.make_async_copy(wout_hbm.at[layer, cols, :], wo.at[slot], wo_sem.at[slot]))

    def slice_copies(m):
        rows = pl.ds(pl.multiple_of(m * MT, MT), MT)
        return (pltpu.make_async_copy(gh_hbm.at[rows], gh.at[rows], first_sem.at[0, m]),
                pltpu.make_async_copy(u_hbm[layers - 1].at[rows, pl.ds(0, HC)], ub.at[0, rows], first_sem.at[1, m]),
                pltpu.make_async_copy(h_hbm[layers - 1].at[rows], hb.at[0, rows], first_sem.at[2, m]))

    def start_chunk(i):
        for k in range(layers):
            @pl.when(layers - 1 - i // per_layer == k)
            def _():
                pre_of(i, u_hbm[k]).start()
        for copy in weights_of(i):
            copy.start()

    def start_hidden(j):
        for k in range(layers):
            @pl.when(layers - 1 - j == k)
            def _():
                pltpu.make_async_copy(h_hbm[k], hb.at[lax.rem(j, 2)], h_sem.at[lax.rem(j, 2)]).start()

    def tile(with_back, m, slot, hslot):
        rows = pl.ds(pl.multiple_of(m * MT, MT), MT)
        u = ub[slot, rows, :].astype(F32)
        u2 = u * u
        t = jnp.tanh(u * (GELU_C + GELU_CK * u2))
        cdf = 0.5 + 0.5 * t
        act = (u * cdf).astype(BF16)
        slope = cdf + (u * (1.0 - t * t)) * (0.5 * GELU_C + 1.5 * GELU_CK * u2)
        g = gh[rows, :]
        g_act = lax.dot_general(g, wo[slot], COLS_BOTH, preferred_element_type=F32).astype(BF16)
        acc_out[...] += lax.dot_general(act, g, ROWS_BOTH, preferred_element_type=F32)
        g_pre = (g_act.astype(F32) * slope).astype(BF16)
        acc_in[...] += lax.dot_general(hb[hslot, rows, :], g_pre, ROWS_BOTH, preferred_element_type=F32)
        if with_back:
            back[rows, :] += lax.dot_general(g_pre, wi[slot], COLS_BOTH, preferred_element_type=F32)

    for copy in weights_of(0):
        copy.start()

    @pl.loop(0, tokens // MT)
    def _(m):
        for copy in slice_copies(m):
            copy.start()

    def chunk_step(i, carry):
        slot = lax.rem(i, 2)
        j = i // per_layer
        hslot = lax.rem(j, 2)

        @pl.when(i + 1 < chunks)
        def _():
            start_chunk(i + 1)

        @pl.when(lax.rem(i, per_layer) == 0)
        def _():
            @pl.when(j > 0)
            def _():
                pltpu.make_async_copy(h_hbm[0], hb.at[hslot], h_sem.at[hslot]).wait()

            @pl.when(j + 1 < layers)
            def _():
                start_hidden(j + 1)

            @pl.loop(0, tokens // MT)
            def _(m):
                back[pl.ds(pl.multiple_of(m * MT, MT), MT), :] = jnp.zeros((MT, width), F32)

        acc_out[...] = jnp.zeros_like(acc_out)
        acc_in[...] = jnp.zeros_like(acc_in)
        for copy in weights_of(i):
            copy.wait()

        @pl.when(i > 0)
        def _():
            pre_of(i, u_hbm[0]).wait()

        @pl.loop(0, 4)
        def _(q):
            t = 2 * i + q // 2
            pl.when(lax.rem(q, 2) == 0)(lambda: halving_side(t))
            pl.when(lax.rem(q, 2) == 1)(lambda: doubling_side(t))
            per_quarter = tokens // MT // 4

            @pl.when(i == 0)
            def _():
                @pl.loop(0, per_quarter)
                def _(m):
                    for copy in slice_copies(q * per_quarter + m):
                        copy.wait()

            def tiles(with_back):
                @pl.loop(0, per_quarter)
                def _(m):
                    tile(with_back, q * per_quarter + m, slot, hslot)

            pl.when(j < layers - 1)(lambda: tiles(True))
            pl.when(j == layers - 1)(lambda: tiles(False))

        s_out, s_in = lax.rem(2 * i, 3), lax.rem(2 * i + 1, 3)
        for half in range(2):
            for p in range(3):
                grads[s_out, half, p] = acc_out[half * BLK:(half + 1) * BLK, p * BLK:(p + 1) * BLK].astype(BF16)
                grads[s_in, half, p] = acc_in[p * BLK:(p + 1) * BLK, half * BLK:(half + 1) * BLK].astype(BF16)

        @pl.when(jnp.logical_and(lax.rem(i, per_layer) == per_layer - 1, i + 1 < chunks))
        def _():
            @pl.loop(0, tokens // MT)
            def _(m):
                rows = pl.ds(pl.multiple_of(m * MT, MT), MT)
                gh[rows, :] = gh[rows, :] + back[rows, :].astype(BF16)
        return carry

    lax.fori_loop(0, chunks, chunk_step, 0)

    def drain(t, carry):
        halving_side(t)
        doubling_side(t)
        return carry

    lax.fori_loop(pieces, pieces + DELAY + 8, drain, 0)


def forward_kernel(layers, coef, *refs):
    (x_hbm, t_hbm, win_hbm, wout_hbm), rest = refs[:4], refs[4:]
    gh_hbm, rest = rest[0], rest[1:]
    h_hbm, rest = rest[:layers - 1], rest[layers - 1:]
    u_hbm, rest = rest[:layers], rest[layers:]
    win, wout, hid, branch, ubuf, hbuf, tbuf, gbuf, w_sem, x_sem, t_sem, u_sem, h_sem, g_sem = rest
    tokens = x_hbm.shape[0]
    chunks = win.shape[2] // FC
    tiles = tokens // FT

    def weight_copies(k):
        return (pltpu.make_async_copy(win_hbm.at[k], win.at[k], w_sem.at[k, 0]),
                pltpu.make_async_copy(wout_hbm.at[k], wout.at[k], w_sem.at[k, 1]))

    def tile_rows(r):
        return pl.ds(pl.multiple_of(r * FT, FT), FT)

    def load_x(r):
        return pltpu.make_async_copy(x_hbm.at[tile_rows(r)], hid.at[lax.rem(r, 2)], x_sem.at[lax.rem(r, 2)])

    def load_t(r):
        return pltpu.make_async_copy(t_hbm.at[tile_rows(r)], tbuf, t_sem.at[0])

    def step_of(r, k, c):
        return (r * layers + k) * chunks + c

    def store_u(r, k, c):
        cols = pl.ds(pl.multiple_of(c * FC, FC), FC)
        slot = lax.rem(step_of(r, k, c), 2)
        return pltpu.make_async_copy(ubuf.at[slot], u_hbm[k].at[tile_rows(r), cols], u_sem.at[slot])

    def store_h(r, k):
        return pltpu.make_async_copy(hbuf.at[k % 2], h_hbm[k].at[tile_rows(r)], h_sem.at[k % 2])

    def store_g(r):
        return pltpu.make_async_copy(gbuf, gh_hbm.at[tile_rows(r)], g_sem.at[0])

    load_x(0).start()
    for k in range(layers):
        for copy in weight_copies(k):
            copy.start()

    @pl.loop(0, tiles)
    def _(r):
        cur = lax.rem(r, 2)
        load_x(r).wait()
        load_t(r).start()

        @pl.when(r + 1 < tiles)
        def _():
            load_x(r + 1).start()

        for k in range(layers):
            @pl.when(r == 0)
            def _():
                for copy in weight_copies(k):
                    copy.wait()

            branch[...] = hid[cur].astype(F32)

            @pl.loop(0, chunks)
            def _(c):
                @pl.when(step_of(r, k, c) >= 2)
                def _():
                    store_u(r, k, c).wait()
                cols = pl.ds(pl.multiple_of(c * FC, FC), FC)
                pre = jnp.dot(hid[cur], win[k, :, cols], preferred_element_type=F32).astype(BF16)
                ubuf[lax.rem(step_of(r, k, c), 2)] = pre
                u = pre.astype(F32)
                t = jnp.tanh(u * (GELU_C + GELU_CK * (u * u)))
                act = (u * (0.5 + 0.5 * t)).astype(BF16)
                branch[...] += jnp.dot(act, wout[k, cols, :], preferred_element_type=F32)
                store_u(r, k, c).start()

            new = branch[...].astype(BF16)
            if k < layers - 1:
                @pl.when(r * layers + k >= 2)
                def _():
                    store_h(r, k).wait()
                hid[cur] = new
                hbuf[k % 2] = new
                store_h(r, k).start()
            else:
                load_t(r).wait()

                @pl.when(r > 0)
                def _():
                    store_g(r).wait()
                gbuf[...] = ((new.astype(F32) - tbuf[...].astype(F32)) * coef).astype(BF16)
                store_g(r).start()

    for slot in range(2):
        cols = pl.ds(0, FC)
        pltpu.make_async_copy(ubuf.at[slot], u_hbm[0].at[pl.ds(0, FT), cols], u_sem.at[slot]).wait()
    for k in range(min(2, layers - 1)):
        store_h(tiles - 1, k).wait()
    store_g(tiles - 1).wait()


def copy_kernel(a_ref, b_ref, c_ref, d_ref):
    c_ref[...] = a_ref[...]
    d_ref[...] = b_ref[...]


def solution(mesh):
    axis = mesh.axis_names[0]

    def grad_program(tokens, targets, w_in, w_out):
        total_tokens, width = tokens.shape
        target_scale = 1.0 + 16.0 * math.sqrt(total_tokens / width)
        loss_coef = 1.0 / (target_scale * math.sqrt(total_tokens))
        layers, _, hidden_width = w_in.shape

        def device_step(tok_rows, tgt_rows, w_first, w_second):
            rows = tok_rows.shape[0]
            any_spec = pl.BlockSpec(memory_space=pl.ANY)
            dma = pltpu.SemaphoreType.DMA
            row_shape = jax.ShapeDtypeStruct((rows, width), BF16)
            pre_shape = jax.ShapeDtypeStruct((rows, hidden_width), BF16)
            forward = pl.pallas_call(
                functools.partial(forward_kernel, layers, loss_coef),
                out_shape=[row_shape] * layers + [pre_shape] * layers,
                in_specs=[any_spec] * 4,
                out_specs=[any_spec] * (2 * layers),
                scratch_shapes=[
                    pltpu.VMEM(w_first.shape, BF16), pltpu.VMEM(w_second.shape, BF16),
                    pltpu.VMEM((2, FT, width), BF16), pltpu.VMEM((FT, width), F32),
                    pltpu.VMEM((2, FT, FC), BF16), pltpu.VMEM((2, FT, width), BF16),
                    pltpu.VMEM((FT, width), BF16), pltpu.VMEM((FT, width), BF16),
                    dma((layers, 2)), dma((2,)), dma((1,)), dma((2,)), dma((2,)), dma((1,)),
                ],
                compiler_params=pltpu.CompilerParams(vmem_limit_bytes=67043328),
                cost_estimate=pl.CostEstimate(flops=4 * rows * width * hidden_width * layers,
                                              bytes_accessed=200 * 2**20, transcendentals=0),
                name="forward",
            )(tok_rows, tgt_rows, w_first, w_second)
            grad_h, saved_h, saved_u = forward[0], [tok_rows, *forward[1:layers]], forward[layers:]

            flops = 8 * rows * width * hidden_width * layers
            summed_in, summed_out = pl.pallas_call(
                functools.partial(backward_kernel, axis, layers),
                out_shape=(jax.ShapeDtypeStruct(w_first.shape, F32), jax.ShapeDtypeStruct(w_second.shape, F32)),
                in_specs=[any_spec] * (3 + 2 * layers),
                out_specs=(any_spec, any_spec),
                scratch_shapes=[
                    pltpu.VMEM((rows, width), BF16),
                    pltpu.VMEM((2, rows, width), BF16),
                    pltpu.VMEM((rows, width), F32),
                    pltpu.VMEM((2, rows, HC), BF16),
                    pltpu.VMEM((2, width, HC), BF16),
                    pltpu.VMEM((2, HC, width), BF16),
                    pltpu.VMEM((HC, width), F32),
                    pltpu.VMEM((width, HC), F32),
                    pltpu.VMEM((3, 2, 3, BLK, BLK), BF16),
                    pltpu.VMEM((2, 3, BLK, BLK), BF16),
                    pltpu.VMEM((NS, 3, BLK // 2, BLK), F32),
                    pltpu.VMEM((3, BLK // 2, BLK), F32),
                    pltpu.VMEM((NF, 3, BLK, BLK), F32),
                    pltpu.VMEM((2, 3, BLK // 2, BLK), F32),
                    pltpu.VMEM((2, 3, BLK // 4, BLK), F32),
                    pltpu.VMEM((2, 3, BLK // 8, BLK), F32),
                    dma((3, rows // MT)), dma((2,)), dma((2,)), dma((2,)), dma((2,)),
                    dma((2,)), dma((2,)),
                    dma((3, 2, 3)), dma((3, 2, 3)), dma((3, 2, 3)), dma((3, 2, 3)),
                    dma((2, 3)), dma((2, 3)), dma((2, 3)),
                ],
                compiler_params=pltpu.CompilerParams(
                    collective_id=0, has_side_effects=True, vmem_limit_bytes=67043328),
                cost_estimate=pl.CostEstimate(flops=flops, bytes_accessed=300 * 2**20, transcendentals=0),
                name="backward_allreduce",
            )(grad_h, *saved_h, *saved_u, w_first, w_second)

            cut = 6
            steps = cut * layers
            in_block = pl.BlockSpec((1, width // cut, hidden_width), lambda s: (s // cut, s % cut, 0))
            out_block = pl.BlockSpec((1, hidden_width // cut, width), lambda s: (s // cut, s % cut, 0))
            return pl.pallas_call(
                copy_kernel,
                grid=(steps,),
                out_shape=(jax.ShapeDtypeStruct(w_first.shape, F32), jax.ShapeDtypeStruct(w_second.shape, F32)),
                in_specs=[in_block, out_block],
                out_specs=(in_block, out_block),
                compiler_params=pltpu.CompilerParams(vmem_limit_bytes=60 * 2**20),
                name="copy_out",
            )(summed_in, summed_out)

        return jax.shard_map(device_step, mesh=mesh, in_specs=(P(axis), P(axis), P(), P()), out_specs=(P(), P()), check_vma=False)(tokens, targets, w_in, w_out)

    return grad_program
```
